32 devices in a mesh: groups: 2 (over y), seq: 16 (over z, x, core).
Axes of the slice: x: 2, y: 2, z: 4, core: 2. Of those that a mesh axis runs over, the one named last changes fastest.
Arguments:
- queries: bfloat16 [8192, 768], P(('groups', 'seq')), parts along dimension 0, may hold values from -30 to 30
- keys: bfloat16 [8192, 128], P(('groups', 'seq')), parts along dimension 0, may hold values from -14 to 14
- values: bfloat16 [8192, 128], P(('groups', 'seq')), parts along dimension 0, may hold values from -6 to 6
- span_ids: int32 [64], P(('groups', 'seq')), parts along dimension 0, may hold values from 0 to 31, each once
- lengths: int32 [16], P('groups'), parts along dimension 0, may hold values from 1 to 16, 32 in all
- page_dest: int32 [64], P('groups'), parts along dimension 0, may hold values from 0 to 31, each once
Outputs:
- context: bfloat16 [8192, 768], P(('groups', 'seq')), parts along dimension 0
- paged_kv: bfloat16 [64, 128, 256], P(('groups', 'seq')), parts along dimension 0
The draws below stay inside these ranges and needn't reach their ends.
There are 2 independent parts, one for each index of `groups`. The reference program is written for one: setup_inputs(seed, part) draws one part's arguments, and reference() takes and returns one part's arrays. A program takes and returns all parts, laid end to end along the dimension named above; each array names one. Nothing has to cross between parts.
Inputs may be any that keep to these rules, and one draw needn't show every extreme that they name: `span_ids`: every packed span number appears once over the whole array. The lengths sum to 32, and one of them equals 16. `page_dest`: every page slot receives exactly one span.
All inputs are finite; a program needn't handle non-finite values.
Results may differ from the reference program's by a relative error of at most 0.012.
The reference program's roundings to bfloat16 on the way count: a program that leaves them out, or rounds other values in their place, can miss the bound.
Values may be sent and summed in bfloat16 or wider, within the bound.
A program may use at most 128 MiB of HBM per device.

```python
import math
import jax
import jax.numpy as jnp
import numpy as np
from jax import lax

HD = 128
QH = 6
SPAN = 128
NSEQ = 8
SPANS = 32
TOKENS = 4096
MOST = 16


def draw_queries(key, part):
    inner = jax.random.fold_in(key, 101)
    base = jnp.clip(3.0 * jax.random.normal(inner, (TOKENS, QH * HD), jnp.float32), -15.0, 15.0)
    return base.astype(jnp.bfloat16)


def draw_keys(key, part):
    inner = jax.random.fold_in(key, 202)
    base = jnp.clip(jax.random.normal(inner, (TOKENS, HD), jnp.float32), -4.0, 4.0)
    return base.astype(jnp.bfloat16)


def steps_of(own_key, shape, pieces, smallest, largest):
    gain, own = 1.0, jax.random.fold_in(own_key, 6)
    for axis_at, shards_of in pieces:
        draws = jnp.exp(jax.random.uniform(jax.random.fold_in(own, axis_at), (shards_of,), jnp.float32, smallest / len(pieces), largest / len(pieces)))
        gain = gain * jnp.repeat(draws, shape[axis_at] // shards_of).reshape([-1 if axis == axis_at else 1 for axis in range(len(shape))])
    return gain


def profile(number_of, total, bound, slope):
    weights = [(1 << 20) // math.isqrt(standing ** slope) + 1 for standing in range(2, number_of + 1)]
    rest, counts = total - bound - (number_of - 1), [1] * (number_of - 1)
    while rest > 0:
        free = [i for i in range(number_of - 1) if counts[i] < bound]
        pool, remaining = sum([weights[i] for i in free]), rest
        for i in free:
            addition = min(bound - counts[i], max(1, remaining * weights[i] // pool), rest)
            counts[i] = counts[i] + addition
            rest = rest - addition
    return np.array([bound] + counts)


def uneven(stream_key, amount, total, most, skew):
    if amount == 2:
        one = jax.random.randint(stream_key, (), max(1, total - most), min(most, total - 1) + 1)
        return jnp.stack([one, total - one])
    sizes = jnp.asarray(profile(amount, total, most, skew), jnp.int32)
    couples = (amount - 1) // 2
    source_of, sink = sizes[1:1 + 2 * couples:2], sizes[2:2 + 2 * couples:2]
    room = jnp.minimum(source_of - 1, most - sink)
    shifted = jax.random.randint(jax.random.fold_in(stream_key, 1), (couples,), 0, 1 << 20) % (room + 1)
    sizes = sizes.at[1:1 + 2 * couples:2].set(source_of - shifted).at[2:2 + 2 * couples:2].set(sink + shifted)
    return sizes[jax.random.permutation(jax.random.fold_in(stream_key, 2), amount)]


def gaussian(rng, extent, scale, most, split=(), kind=jnp.bfloat16):
    gain = steps_of(rng, extent, split, -0.22, 0.18) if split else 1.0
    result = jax.random.normal(rng, extent, jnp.float32) * scale * gain
    return jnp.minimum(jnp.maximum(result, -most), most).astype(kind)


def setup_inputs(seed: int = 0, part: int = 0) -> dict:
    streams_of = jax.random.split(jax.random.key(seed), 7)
    part_splits = jax.random.split(jax.random.fold_in(streams_of[6], part), 7)
    return {
        "queries": draw_queries(jax.random.fold_in(jax.random.fold_in(streams_of[6], part), 71), part),
        "keys": draw_keys(jax.random.fold_in(jax.random.fold_in(streams_of[6], part), 71), part),
        "values": gaussian(part_splits[2], (TOKENS, HD), 1.0, 6.0, ((0, 16),)),
        "span_ids": jax.random.permutation(part_splits[3], SPANS).astype(jnp.int32),
        "lengths": uneven(part_splits[4], NSEQ, SPANS, MOST, 2).astype(jnp.int32),
        "page_dest": jax.random.permutation(part_splits[5], SPANS).astype(jnp.int32),
    }


THETA = 1000000.0
NEG = -1e30


def rotate(x, pos):
    half = HD // 2
    freq = THETA ** (-(jnp.arange(half, dtype=jnp.float32) * 2.0 / HD))
    angle = pos[:, None] * freq[None, :]
    cosine = jnp.cos(angle)[:, None, :]
    sine = jnp.sin(angle)[:, None, :]
    first = x[..., :half]
    second = x[..., half:]
    return jnp.concatenate([first * cosine - second * sine, second * cosine + first * sine], axis=-1)


def locate(tokens, lengths):
    span_of = tokens // SPAN
    ends = jnp.cumsum(lengths)
    start_span = jnp.sum(jnp.where(ends[None, :] <= span_of[:, None], lengths[None, :], 0), axis=1)
    start = (start_span * SPAN).astype(jnp.int32)
    return start, (tokens - start).astype(jnp.int32)


def reference(queries, keys, values, span_ids, lengths, page_dest):
    rows = jnp.arange(TOKENS, dtype=jnp.int32)
    tokens = (span_ids[rows // SPAN] * SPAN + rows % SPAN).astype(jnp.int32)
    start, pos = locate(tokens, lengths)
    posf = pos.astype(jnp.float32)
    q_rot = rotate(queries.astype(jnp.float32).reshape(TOKENS, QH, HD), posf).astype(jnp.bfloat16)
    k_rot = rotate(keys.astype(jnp.float32)[:, None, :], posf)[:, 0, :].astype(jnp.bfloat16)
    q_blocks = q_rot.reshape(SPANS, SPAN * QH, HD)
    q_tok = jnp.repeat(tokens, QH).reshape(SPANS, SPAN * QH)
    q_start = jnp.repeat(start, QH).reshape(SPANS, SPAN * QH)
    scale = 1.0 / (HD ** 0.5)

    def one_span(item):
        block, qtok, qstart = item
        scores = jnp.dot(block, k_rot.T, preferred_element_type=jnp.float32) * scale
        mask = (tokens[None, :] <= qtok[:, None]) & (tokens[None, :] >= qstart[:, None])
        best = jnp.max(jnp.where(mask, scores, NEG), axis=1)
        weights = jnp.where(mask, jnp.exp(scores - best[:, None]), 0.0)
        total = jnp.sum(weights, axis=1)
        mixed = jnp.dot(weights.astype(jnp.bfloat16), values, preferred_element_type=jnp.float32)
        return (mixed / total[:, None]).astype(jnp.bfloat16)

    context = lax.map(one_span, (q_blocks, q_tok, q_start)).reshape(TOKENS, QH * HD)
    packed = jnp.concatenate([k_rot, values], axis=1).reshape(SPANS, SPAN, 2 * HD)
    slots = page_dest[span_ids].astype(jnp.int32)
    paged_kv = jnp.zeros((SPANS, SPAN, 2 * HD), jnp.bfloat16).at[slots].set(packed)
    return context, paged_kv
```

```python
import functools
import math

import jax
import jax.numpy as jnp
import numpy as np
from jax import lax
from jax.experimental import pallas as pl
from jax.experimental.pallas import tpu as pltpu
from jax.sharding import PartitionSpec as P

HD = 128
QH = 6
SPAN = 128
THETA = 1000000.0
NEG = -1e30
MESH = pl.DeviceIdType.MESH
VMEM = pltpu.VMEM
SMEM = pltpu.SMEM


def tables(span_total):
    half = HD // 2
    freq = (THETA ** (-(np.arange(half) * 2.0 / HD))).astype(np.float32).astype(np.float64)
    sign = np.concatenate([-np.ones(half), np.ones(half)])

    def pair(places):
        angle = np.tile(places[:, None] * freq[None, :], (1, 2))
        return np.stack([np.cos(angle), np.sin(angle) * sign]).astype(np.float32)

    near = pair(np.arange(SPAN, dtype=np.float64))
    far = pair(np.arange(span_total, dtype=np.float64) * SPAN).transpose(1, 0, 2)
    return near, np.ascontiguousarray(far)


def start_of(span, lengths, count):
    ends = jnp.int32(0)
    start = jnp.int32(0)
    for i in range(count):
        size = lengths[i]
        ends = ends + size
        start = start + jnp.where(ends <= span, size, 0)
    return start


def layout_of(n):
    cores = 2 if n % 2 == 0 else 1
    chips = n // cores
    wide = 1
    while (wide + 1) ** 3 <= chips:
        wide += 1
    while chips % wide:
        wide -= 1
    return cores, wide, chips // wide


def gather_kernel(
    n, per_rank, histories,
    span_ids, lengths, near, far, queries, keys, values,
    kv, meta, q_rot,
    send_sem, recv_sem,
):
    cores, wide, deep = layout_of(n)
    me = lax.axis_index("seq")
    group = lax.axis_index("groups")
    c = lax.rem(me, cores)
    x = lax.rem(me // cores, wide)
    z = me // (cores * wide)
    items = per_rank + 1

    def at(zz, xx):
        return (zz * wide + xx) * cores + c

    barrier = pltpu.get_barrier_semaphore()
    neighbours = [
        (z < deep - 1, me + wide * cores),
        (z > 0, me - wide * cores),
        (x < wide - 1, me + cores),
        (x > 0, me - cores),
    ]
    if cores == 2:
        neighbours.append((None, me + 1 - 2 * c))
    greeted = jnp.int32(0)
    for there, other in neighbours:
        def greet(other=other):
            pl.semaphore_signal(barrier, inc=1, device_id=(group, other), device_id_type=MESH)
        if there is None:
            greet()
            greeted = greeted + 1
        else:
            pl.when(there)(greet)
            greeted = greeted + there.astype(jnp.int32)

    factors = []
    for slot in range(per_rank):
        span = span_ids[slot]
        place = span - start_of(span, lengths, histories)
        base = far[pl.ds(place, 1)]
        c2, s2 = base[0, 0:1, :], base[0, 1:2, :]
        c1, s1 = near[0], near[1]
        factors.append((c1 * c2 - s1 * s2, s1 * c2 + c1 * s2))

    def rotate(rows, slot):
        cosine, sine = factors[slot]
        rows = rows.astype(jnp.float32)
        return (rows * cosine + pltpu.roll(rows, HD // 2, 1) * sine).astype(jnp.bfloat16)

    lane = lax.broadcasted_iota(jnp.int32, (1, 128), 1)
    note = jnp.zeros((1, 128), jnp.int32)
    for slot in range(per_rank):
        note = jnp.where(lane == slot, span_ids[slot], note)
    meta[me] = note
    for slot in range(per_rank):
        rows = slice(slot * SPAN, (slot + 1) * SPAN)
        kv[me * per_rank + slot, :, HD:] = values[rows, :]
        kv[me * per_rank + slot, :, :HD] = rotate(keys[rows, :], slot)

    pl.semaphore_wait(barrier, greeted)

    def ref_of(device, k):
        return kv.at[device * per_rank + k] if k < per_rank else meta.at[device]

    pending = []

    def both(a, b):
        return a if b is None else (b if a is None else jnp.logical_and(a, b))

    def send(device, k, target, there):
        number = len(pending)
        ref = ref_of(device, k)
        copy = pltpu.make_async_remote_copy(
            src_ref=ref, dst_ref=ref,
            send_sem=send_sem.at[number], recv_sem=recv_sem.at[device * items + k],
            device_id=(group, target), device_id_type=MESH,
        )
        if there is None:
            copy.start()
            pending.append((None, copy))
        else:
            pl.when(there)(copy.start)
            pending.append((there, copy))

    def arrive(device, k, there):
        ref = ref_of(device, k)
        copy = pltpu.make_async_remote_copy(
            src_ref=ref, dst_ref=ref,
            send_sem=send_sem.at[0], recv_sem=recv_sem.at[device * items + k],
            device_id=(group, me), device_id_type=MESH,
        )
        if there is None:
            copy.wait_recv()
        else:
            pl.when(there)(copy.wait_recv)

    def up(device, k, there):
        send(device, k, me + wide * cores, both(there, z < deep - 1))

    def down(device, k, there):
        send(device, k, me - wide * cores, both(there, z > 0))

    def right(device, k, there):
        send(device, k, me + cores, both(there, x < wide - 1))

    def left(device, k, there):
        send(device, k, me - cores, both(there, x > 0))

    def partner(device, k, there):
        if cores == 2:
            send(device, k, me + 1 - 2 * c, there)

    balanced = wide == 2 and deep >= 4
    late = per_rank - 1

    for k in range(items):
        up(me, k, None)
        down(me, k, None)
        right(me, k, None)
        left(me, k, None)
    for k in range(items):
        partner(me, k, None)

    for slot in range(per_rank):
        rows = slice(slot * SPAN, (slot + 1) * SPAN)
        for head in range(QH):
            q_rot[slot, head * SPAN:(head + 1) * SPAN, :] = rotate(
                queries[rows, head * HD:(head + 1) * HD], slot
            )

    for d in range(deep):
        if d < deep - 1:
            far_by = d + 1
            for k in range(items):
                for sign in (-1, 1):
                    row = z + sign * far_by
                    there = row >= 0 if sign < 0 else row < deep
                    device = at(row, x)
                    arrive(device, k, there)
                    (up if sign < 0 else down)(device, k, there)
                    across = there
                    if balanced and far_by == 1:
                        if sign < 0:
                            along = row == 0
                            if k == late:
                                along = jnp.logical_or(along, row == deep - 2)
                        else:
                            along = row == deep - 1
                            if k == late:
                                along = jnp.logical_or(along, row == 1)
                        across = jnp.logical_and(there, jnp.logical_not(along))
                    right(device, k, across)
                    left(device, k, across)
                    partner(device, k, there)
        for k in range(items):
            for sign in ((-1, 1) if d else (1,)):
                row = z + sign * d
                row_there = None if d == 0 else (row >= 0 if sign < 0 else row < deep)
                for e in range(1, wide):
                    for side in (-1, 1):
                        column = x + side * e
                        there = both(row_there, column >= 0 if side < 0 else column < wide)
                        device = at(row, column)
                        arrive(device, k, there)
                        if e < wide - 1:
                            (right if side < 0 else left)(device, k, there)
                        if balanced and d == 0:
                            rise, fall = z == 0, z == deep - 1
                            if k == late:
                                rise = jnp.logical_or(rise, z == deep - 2)
                                fall = jnp.logical_or(fall, z == 1)
                            up(device, k, both(there, rise))
                            down(device, k, both(there, fall))
                        partner(device, k, there)

    if cores == 2:
        def drain(chip, carry):
            device = chip * cores + 1 - c
            for k in range(items):
                arrive(device, k, None)
            return carry

        lax.fori_loop(0, n // cores, drain, 0)
    for there, copy in pending:
        if there is None:
            copy.wait_send()
        else:
            pl.when(there)(copy.wait_send)


def sends_of(n, per_rank):
    cores, wide, deep = layout_of(n)
    items = per_rank + 1
    total = items * 5 + items * 2 * (deep - 1) * 4
    total += items * (2 * deep - 1) * 2 * (wide - 1) * 4
    return total


def attend_kernel(
    per_rank, span_total, histories, tile, axis,
    span_ids, lengths, page_dest, meta, q_rot, kv,
    context, paged,
    where_is, scores, best, total, accum,
):
    rank = lax.axis_index(axis)
    devices = span_total // per_rank
    gain = math.log2(math.e) / math.sqrt(HD)

    for device in range(devices):
        for k in range(per_rank):
            where_is[meta[device, 0, k]] = device * per_rank + k

    for slot in range(per_rank):
        wanted = rank * per_rank + slot
        found = jnp.int32(0)
        for j in range(span_total):
            found = jnp.where(page_dest[j] == wanted, j, found)
        paged[slot] = kv[where_is[found]]

    def joined(cur, first, width, columns):
        blocks = [kv[where_is[cur - first - j], :, columns] for j in range(width)]
        return blocks[0] if width == 1 else jnp.concatenate(blocks, axis=0)

    def one(item, carry):
        slot = item // (QH * SPAN // tile)
        row0 = pl.multiple_of(lax.rem(item, QH * SPAN // tile) * tile, tile)
        cur = span_ids[slot]
        behind = cur - start_of(cur, lengths, histories)
        fours = behind // 4
        twos = lax.rem(behind, 4) // 2
        ones = lax.rem(behind, 2)
        query = q_rot[slot, pl.ds(row0, tile), :]

        def dots(first, width):
            return lax.dot_general(
                query, joined(cur, first, width, slice(0, HD)),
                (((1,), (1,)), ((), ())), preferred_element_type=jnp.float32,
            )

        def score(first, width):
            block = dots(first, width)
            top = best[...]
            for j in range(width):
                piece = block[:, j * SPAN:(j + 1) * SPAN]
                scores[first + j] = piece
                top = jnp.maximum(top, piece)
            best[...] = top

        def weigh(first, width, fresh=False):
            top = best[...]
            parts, summed = [], None
            for j in range(width):
                part = jnp.exp2((scores[first + j] - top) * gain)
                summed = part if summed is None else summed + part
                parts.append(part.astype(jnp.bfloat16))
            low = parts[0] if width == 1 else jnp.concatenate(parts, axis=1)
            mixed = jnp.dot(
                low, joined(cur, first, width, slice(HD, 2 * HD)), preferred_element_type=jnp.float32
            )
            if fresh:
                total[...] = summed
                accum[...] = mixed
            else:
                total[...] += summed
                accum[...] += mixed

        def sweep(step):
            def body(i, c):
                step(1 + i * 4, 4)
                return c

            lax.fori_loop(0, fours, body, 0)

            @pl.when(twos == 1)
            def _():
                step(1 + fours * 4, 2)

            @pl.when(ones == 1)
            def _():
                step(1 + fours * 4 + twos * 2, 1)

        own = dots(0, 1)
        row = lax.rem(lax.broadcasted_iota(jnp.int32, (tile, SPAN), 0), SPAN)
        col = lax.broadcasted_iota(jnp.int32, (tile, SPAN), 1)
        own = jnp.where(col <= row, own, NEG)
        scores[0] = own
        best[...] = own
        sweep(score)
        best[...] = jnp.broadcast_to(jnp.max(best[...], axis=1, keepdims=True), (tile, SPAN))
        weigh(0, 1, fresh=True)
        sweep(weigh)
        result = accum[...] / jnp.sum(total[...], axis=1, keepdims=True)
        result = result.astype(jnp.bfloat16)
        rows = pl.ds(pl.multiple_of(slot * SPAN, SPAN), SPAN)
        heads = tile // SPAN
        if heads == QH:
            for head in range(QH):
                context[rows, head * HD:(head + 1) * HD] = result[head * SPAN:(head + 1) * SPAN]
        else:
            for head in range(heads):
                place = pl.ds(pl.multiple_of(row0 // SPAN * HD + head * HD, HD), HD)
                context[rows, place] = result[head * SPAN:(head + 1) * SPAN]
        return carry

    lax.fori_loop(0, per_rank * (QH * SPAN // tile), one, 0)


def on_device(n, queries, keys, values, span_ids, lengths, page_dest):
    per_rank = span_ids.shape[0]
    span_total = page_dest.shape[0]
    histories = lengths.shape[0]
    near, far = tables(span_total)
    vmem, smem = pl.BlockSpec(memory_space=VMEM), pl.BlockSpec(memory_space=SMEM)
    items = per_rank + 1
    kv, meta, q_rot = pl.pallas_call(
        functools.partial(gather_kernel, n, per_rank, histories),
        out_shape=(
            jax.ShapeDtypeStruct((span_total, SPAN, 2 * HD), jnp.bfloat16),
            jax.ShapeDtypeStruct((n, 1, 128), jnp.int32),
            jax.ShapeDtypeStruct((per_rank, QH * SPAN, HD), jnp.bfloat16),
        ),
        in_specs=[smem, smem] + [vmem] * 5,
        out_specs=(vmem, vmem, vmem),
        scratch_shapes=[
            pltpu.SemaphoreType.DMA((sends_of(n, per_rank),)),
            pltpu.SemaphoreType.DMA((n * items,)),
        ],
        compiler_params=pltpu.CompilerParams(collective_id=0, has_side_effects=True),
        name="gather",
    )(span_ids, lengths, jnp.asarray(near), jnp.asarray(far), queries, keys, values)
    reach = span_total // 2
    tile = QH * SPAN
    for parts in (1, 2, 3, 6):
        tile = QH * SPAN // parts
        if tile * reach * SPAN * 4 <= 16 * 2**20:
            break
    return pl.pallas_call(
        functools.partial(attend_kernel, per_rank, span_total, histories, tile, "seq"),
        out_shape=(
            jax.ShapeDtypeStruct(queries.shape, jnp.bfloat16),
            jax.ShapeDtypeStruct((per_rank, SPAN, 2 * HD), jnp.bfloat16),
        ),
        in_specs=[smem, smem, smem, smem, vmem, vmem],
        out_specs=(vmem, vmem),
        scratch_shapes=[
            SMEM((span_total,), jnp.int32),
            VMEM((reach, tile, SPAN), jnp.float32),
            VMEM((tile, SPAN), jnp.float32),
            VMEM((tile, SPAN), jnp.float32),
            VMEM((tile, HD), jnp.float32),
        ],
        name="attend",
    )(span_ids, lengths, page_dest, meta, q_rot, kv)


def solution(mesh):
    rows = P(("groups", "seq"), None)
    return jax.shard_map(
        functools.partial(on_device, mesh.shape["seq"]),
        mesh=mesh,
        in_specs=(rows, rows, rows, P(("groups", "seq")), P("groups"), P("groups")),
        out_specs=(rows, P(("groups", "seq"), None, None)),
        check_vma=False,
    )
```

```python
import functools
import math

import jax
import jax.numpy as jnp
import numpy as np
from jax import lax
from jax.experimental import pallas as pl
from jax.experimental.pallas import tpu as pltpu
from jax.sharding import PartitionSpec as P

HD = 128
QH = 6
SPAN = 128
THETA = 1000000.0
NEG = -1e30
MESH = pl.DeviceIdType.MESH
VMEM = pltpu.VMEM
SMEM = pltpu.SMEM


def tables(span_total):
    half = HD // 2
    freq = (THETA ** (-(np.arange(half) * 2.0 / HD))).astype(np.float32).astype(np.float64)
    sign = np.concatenate([-np.ones(half), np.ones(half)])

    def pair(places):
        angle = np.tile(places[:, None] * freq[None, :], (1, 2))
        return np.stack([np.cos(angle), np.sin(angle) * sign]).astype(np.float32)

    near = pair(np.arange(SPAN, dtype=np.float64))
    far = pair(np.arange(span_total, dtype=np.float64) * SPAN).transpose(1, 0, 2)
    return near, np.ascontiguousarray(far)


def start_of(span, lengths, count):
    ends = jnp.int32(0)
    start = jnp.int32(0)
    for i in range(count):
        size = lengths[i]
        ends = ends + size
        start = start + jnp.where(ends <= span, size, 0)
    return start


def layout_of(n):
    cores = 2 if n % 2 == 0 else 1
    chips = n // cores
    wide = 1
    while (wide + 1) ** 3 <= chips:
        wide += 1
    while chips % wide:
        wide -= 1
    return cores, wide, chips // wide


def gather_kernel(
    n, per_rank, histories,
    span_ids_hbm, lengths_hbm, near_hbm, far_hbm, queries_hbm, keys_hbm, values_hbm,
    kv, meta, q_rot,
    span_ids, lengths, near, far, queries, keys, load_sem, send_sem, recv_sem,
):
    cores, wide, deep = layout_of(n)
    me = lax.axis_index("seq")
    group = lax.axis_index("groups")
    c = lax.rem(me, cores)
    x = lax.rem(me // cores, wide)
    z = me // (cores * wide)
    items = per_rank + 1

    def at(zz, xx):
        return (zz * wide + xx) * cores + c

    loads = [
        pltpu.make_async_copy(src, dst, load_sem.at[i])
        for i, (src, dst) in enumerate([
            (span_ids_hbm, span_ids), (lengths_hbm, lengths), (far_hbm, far),
            (keys_hbm, keys), (near_hbm, near),
        ] + [
            (values_hbm.at[pl.ds(slot * SPAN, SPAN)],
             kv.at[me * per_rank + slot, :, pl.ds(HD, HD)])
            for slot in range(per_rank)
        ] + [(queries_hbm, queries)])
    ]
    for load in loads:
        load.start()

    barrier = pltpu.get_barrier_semaphore()
    neighbours = [
        (z < deep - 1, me + wide * cores),
        (z > 0, me - wide * cores),
        (x < wide - 1, me + cores),
        (x > 0, me - cores),
    ]
    if cores == 2:
        neighbours.append((None, me + 1 - 2 * c))
    greeted = jnp.int32(0)
    for there, other in neighbours:
        def greet(other=other):
            pl.semaphore_signal(barrier, inc=1, device_id=(group, other), device_id_type=MESH)
        if there is None:
            greet()
            greeted = greeted + 1
        else:
            pl.when(there)(greet)
            greeted = greeted + there.astype(jnp.int32)

    for load in loads[:-1]:
        load.wait()

    factors = []
    for slot in range(per_rank):
        span = span_ids[slot]
        place = span - start_of(span, lengths, histories)
        base = far[pl.ds(place, 1)]
        c2, s2 = base[0, 0:1, :], base[0, 1:2, :]
        c1, s1 = near[0], near[1]
        factors.append((c1 * c2 - s1 * s2, s1 * c2 + c1 * s2))

    def rotate(rows, slot):
        cosine, sine = factors[slot]
        rows = rows.astype(jnp.float32)
        return (rows * cosine + pltpu.roll(rows, HD // 2, 1) * sine).astype(jnp.bfloat16)

    lane = lax.broadcasted_iota(jnp.int32, (1, 128), 1)
    note = jnp.zeros((1, 128), jnp.int32)
    for slot in range(per_rank):
        note = jnp.where(lane == slot, span_ids[slot], note)
    meta[me] = note
    for slot in range(per_rank):
        rows = slice(slot * SPAN, (slot + 1) * SPAN)
        kv[me * per_rank + slot, :, :HD] = rotate(keys[rows, :], slot)

    pl.semaphore_wait(barrier, greeted)

    def ref_of(device, k):
        return kv.at[device * per_rank + k] if k < per_rank else meta.at[device]

    pending = []

    def both(a, b):
        return a if b is None else (b if a is None else jnp.logical_and(a, b))

    def send(device, k, target, there):
        number = len(pending)
        ref = ref_of(device, k)
        copy = pltpu.make_async_remote_copy(
            src_ref=ref, dst_ref=ref,
            send_sem=send_sem.at[number], recv_sem=recv_sem.at[device * items + k],
            device_id=(group, target), device_id_type=MESH,
        )
        if there is None:
            copy.start()
            pending.append((None, copy))
        else:
            pl.when(there)(copy.start)
            pending.append((there, copy))

    def arrive(device, k, there):
        ref = ref_of(device, k)
        copy = pltpu.make_async_remote_copy(
            src_ref=ref, dst_ref=ref,
            send_sem=send_sem.at[0], recv_sem=recv_sem.at[device * items + k],
            device_id=(group, me), device_id_type=MESH,
        )
        if there is None:
            copy.wait_recv()
        else:
            pl.when(there)(copy.wait_recv)

    def up(device, k, there):
        send(device, k, me + wide * cores, both(there, z < deep - 1))

    def down(device, k, there):
        send(device, k, me - wide * cores, both(there, z > 0))

    def right(device, k, there):
        send(device, k, me + cores, both(there, x < wide - 1))

    def left(device, k, there):
        send(device, k, me - cores, both(there, x > 0))

    def partner(device, k, there):
        if cores == 2:
            send(device, k, me + 1 - 2 * c, there)

    balanced = wide == 2 and deep >= 4
    late = per_rank - 1

    for k in range(items):
        down(me, k, None)
        up(me, k, None)
        right(me, k, None)
        left(me, k, None)
    for k in range(items):
        partner(me, k, None)

    loads[-1].wait()
    for slot in range(per_rank):
        rows = slice(slot * SPAN, (slot + 1) * SPAN)
        for head in range(QH):
            q_rot[slot, head * SPAN:(head + 1) * SPAN, :] = rotate(
                queries[rows, head * HD:(head + 1) * HD], slot
            )

    for d in range(deep):
        if d < deep - 1:
            far_by = d + 1
            for k in range(items):
                for sign in (1, -1):
                    row = z + sign * far_by
                    there = row >= 0 if sign < 0 else row < deep
                    device = at(row, x)
                    arrive(device, k, there)
                    (up if sign < 0 else down)(device, k, there)
                    across = there
                    if balanced and k == late:
                        along = jnp.logical_or(row == 0, row == deep - 1)
                        across = jnp.logical_and(there, jnp.logical_not(along))
                    right(device, k, across)
                    left(device, k, across)
                    partner(device, k, there)
        for k in range(items):
            for sign in ((1, -1) if d else (1,)):
                row = z + sign * d
                row_there = None if d == 0 else (row >= 0 if sign < 0 else row < deep)
                for e in range(1, wide):
                    for side in (-1, 1):
                        column = x + side * e
                        there = both(row_there, column >= 0 if side < 0 else column < wide)
                        device = at(row, column)
                        arrive(device, k, there)
                        if e < wide - 1:
                            (right if side < 0 else left)(device, k, there)
                        if balanced and k == late:
                            if d == 0 or sign < 0:
                                up(device, k, both(there, row == 0))
                            if d == 0 or sign > 0:
                                down(device, k, both(there, row == deep - 1))
                        partner(device, k, there)

    if cores == 2:
        def drain(chip, carry):
            device = chip * cores + 1 - c
            for k in range(items):
                arrive(device, k, None)
            return carry

        lax.fori_loop(0, n // cores, drain, 0)
    for there, copy in pending:
        if there is None:
            copy.wait_send()
        else:
            pl.when(there)(copy.wait_send)


def sends_of(n, per_rank):
    cores, wide, deep = layout_of(n)
    items = per_rank + 1
    total = items * 5 + items * 2 * (deep - 1) * 4
    total += items * (2 * deep - 1) * 2 * (wide - 1) * 4
    return total


def attend_kernel(
    per_rank, span_total, histories, tile, axis,
    span_ids_hbm, lengths_hbm, page_dest_hbm, meta, q_rot, kv,
    context, paged,
    span_ids, lengths, page_dest, load_sem, where_is, scores, best, total, accum,
):
    loads = [
        pltpu.make_async_copy(src, dst, load_sem.at[i])
        for i, (src, dst) in enumerate([
            (span_ids_hbm, span_ids), (lengths_hbm, lengths), (page_dest_hbm, page_dest),
        ])
    ]
    for load in loads:
        load.start()
    rank = lax.axis_index(axis)
    devices = span_total // per_rank
    gain = math.log2(math.e) / math.sqrt(HD)

    for device in range(devices):
        for k in range(per_rank):
            where_is[meta[device, 0, k]] = device * per_rank + k

    for load in loads:
        load.wait()
    for slot in range(per_rank):
        wanted = rank * per_rank + slot
        found = jnp.int32(0)
        for j in range(span_total):
            found = jnp.where(page_dest[j] == wanted, j, found)
        paged[slot] = kv[where_is[found]]

    def joined(cur, first, width, columns):
        blocks = [kv[where_is[cur - first - j], :, columns] for j in range(width)]
        return blocks[0] if width == 1 else jnp.concatenate(blocks, axis=0)

    def one(item, carry):
        slot = item // (QH * SPAN // tile)
        row0 = pl.multiple_of(lax.rem(item, QH * SPAN // tile) * tile, tile)
        cur = span_ids[slot]
        behind = cur - start_of(cur, lengths, histories)
        fours = behind // 4
        twos = lax.rem(behind, 4) // 2
        ones = lax.rem(behind, 2)
        query = q_rot[slot, pl.ds(row0, tile), :]

        def dots(first, width):
            return lax.dot_general(
                query, joined(cur, first, width, slice(0, HD)),
                (((1,), (1,)), ((), ())), preferred_element_type=jnp.float32,
            )

        def score(first, width):
            block = dots(first, width)
            top = best[...]
            for j in range(width):
                piece = block[:, j * SPAN:(j + 1) * SPAN]
                scores[first + j] = piece
                top = jnp.maximum(top, piece)
            best[...] = top

        def weigh(first, width, fresh=False):
            top = best[...]
            parts, summed = [], None
            for j in range(width):
                part = jnp.exp2((scores[first + j] - top) * gain)
                summed = part if summed is None else summed + part
                parts.append(part.astype(jnp.bfloat16))
            low = parts[0] if width == 1 else jnp.concatenate(parts, axis=1)
            mixed = jnp.dot(
                low, joined(cur, first, width, slice(HD, 2 * HD)), preferred_element_type=jnp.float32
            )
            if fresh:
                total[...] = summed
                accum[...] = mixed
            else:
                total[...] += summed
                accum[...] += mixed

        def sweep(step):
            def body(i, c):
                step(1 + i * 4, 4)
                return c

            lax.fori_loop(0, fours, body, 0)

            @pl.when(twos == 1)
            def _():
                step(1 + fours * 4, 2)

            @pl.when(ones == 1)
            def _():
                step(1 + fours * 4 + twos * 2, 1)

        own = dots(0, 1)
        row = lax.rem(lax.broadcasted_iota(jnp.int32, (tile, SPAN), 0), SPAN)
        col = lax.broadcasted_iota(jnp.int32, (tile, SPAN), 1)
        own = jnp.where(col <= row, own, NEG)
        scores[0] = own
        best[...] = own
        sweep(score)
        best[...] = jnp.broadcast_to(jnp.max(best[...], axis=1, keepdims=True), (tile, SPAN))
        weigh(0, 1, fresh=True)
        sweep(weigh)
        result = accum[...] / jnp.sum(total[...], axis=1, keepdims=True)
        result = result.astype(jnp.bfloat16)
        rows = pl.ds(pl.multiple_of(slot * SPAN, SPAN), SPAN)
        heads = tile // SPAN
        if heads == QH:
            for head in range(QH):
                context[rows, head * HD:(head + 1) * HD] = result[head * SPAN:(head + 1) * SPAN]
        else:
            for head in range(heads):
                place = pl.ds(pl.multiple_of(row0 // SPAN * HD + head * HD, HD), HD)
                context[rows, place] = result[head * SPAN:(head + 1) * SPAN]
        return carry

    lax.fori_loop(0, per_rank * (QH * SPAN // tile), one, 0)


def in_hbm(array):
    return pltpu.with_memory_space_constraint(array, pltpu.HBM)


def on_device(n, queries, keys, values, span_ids, lengths, page_dest):
    per_rank = span_ids.shape[0]
    span_total = page_dest.shape[0]
    histories = lengths.shape[0]
    near, far = tables(span_total)
    vmem, smem = pl.BlockSpec(memory_space=VMEM), pl.BlockSpec(memory_space=SMEM)
    hbm = pl.BlockSpec(memory_space=pltpu.HBM)
    gathered = span_total * SPAN * 2 * HD * 2
    items = per_rank + 1
    kv, meta, q_rot = pl.pallas_call(
        functools.partial(gather_kernel, n, per_rank, histories),
        out_shape=(
            jax.ShapeDtypeStruct((span_total, SPAN, 2 * HD), jnp.bfloat16),
            jax.ShapeDtypeStruct((n, 1, 128), jnp.int32),
            jax.ShapeDtypeStruct((per_rank, QH * SPAN, HD), jnp.bfloat16),
        ),
        in_specs=[hbm] * 7,
        out_specs=(vmem, vmem, vmem),
        scratch_shapes=[
            SMEM(span_ids.shape, jnp.int32),
            SMEM(lengths.shape, jnp.int32),
            VMEM(near.shape, jnp.float32),
            VMEM(far.shape, jnp.float32),
            VMEM(queries.shape, jnp.bfloat16),
            VMEM(keys.shape, jnp.bfloat16),
            pltpu.SemaphoreType.DMA((6 + per_rank,)),
            pltpu.SemaphoreType.DMA((sends_of(n, per_rank),)),
            pltpu.SemaphoreType.DMA((n * items,)),
        ],
        compiler_params=pltpu.CompilerParams(
            collective_id=0, has_side_effects=True, vmem_limit_bytes=gathered + 6 * 2**20
        ),
        name="gather",
    )(*map(in_hbm, (span_ids, lengths, jnp.asarray(near), jnp.asarray(far), queries, keys, values)))
    reach = span_total // 2
    tile = QH * SPAN
    for parts in (1, 2, 3, 6):
        tile = QH * SPAN // parts
        if tile * reach * SPAN * 4 <= 16 * 2**20:
            break
    return pl.pallas_call(
        functools.partial(attend_kernel, per_rank, span_total, histories, tile, "seq"),
        out_shape=(
            jax.ShapeDtypeStruct(queries.shape, jnp.bfloat16),
            jax.ShapeDtypeStruct((per_rank, SPAN, 2 * HD), jnp.bfloat16),
        ),
        in_specs=[hbm, hbm, hbm, smem, vmem, vmem],
        out_specs=(vmem, vmem),
        scratch_shapes=[
            SMEM(span_ids.shape, jnp.int32),
            SMEM(lengths.shape, jnp.int32),
            SMEM(page_dest.shape, jnp.int32),
            pltpu.SemaphoreType.DMA((3,)),
            SMEM((span_total,), jnp.int32),
            VMEM((reach, tile, SPAN), jnp.float32),
            VMEM((tile, SPAN), jnp.float32),
            VMEM((tile, SPAN), jnp.float32),
            VMEM((tile, HD), jnp.float32),
        ],
        compiler_params=pltpu.CompilerParams(vmem_limit_bytes=gathered + 24 * 2**20),
        name="attend",
    )(*map(in_hbm, (span_ids, lengths, page_dest)), meta, q_rot, kv)


def solution(mesh):
    rows = P(("groups", "seq"), None)
    return jax.shard_map(
        functools.partial(on_device, mesh.shape["seq"]),
        mesh=mesh,
        in_specs=(rows, rows, rows, P(("groups", "seq")), P("groups"), P("groups")),
        out_specs=(rows, P(("groups", "seq"), None, None)),
        check_vma=False,
    )
```

```python
import functools
import math

import jax
import jax.numpy as jnp
import numpy as np
from jax import lax
from jax.experimental import pallas as pl
from jax.experimental.pallas import tpu as pltpu
from jax.sharding import PartitionSpec as P

HD = 128
QH = 6
SPAN = 128
THETA = 1000000.0
NEG = -1e30
MESH = pl.DeviceIdType.MESH
VMEM = pltpu.VMEM
SMEM = pltpu.SMEM


def tables(span_total):
    half = HD // 2
    freq = (THETA ** (-(np.arange(half) * 2.0 / HD))).astype(np.float32).astype(np.float64)
    sign = np.concatenate([-np.ones(half), np.ones(half)])

    def pair(places):
        angle = np.tile(places[:, None] * freq[None, :], (1, 2))
        return np.stack([np.cos(angle), np.sin(angle) * sign]).astype(np.float32)

    near = pair(np.arange(SPAN, dtype=np.float64))
    far = pair(np.arange(span_total, dtype=np.float64) * SPAN).transpose(1, 0, 2)
    return near, np.ascontiguousarray(far)


def start_of(span, lengths, count):
    ends = jnp.int32(0)
    start = jnp.int32(0)
    for i in range(count):
        size = lengths[i]
        ends = ends + size
        start = start + jnp.where(ends <= span, size, 0)
    return start


def layout_of(n):
    cores = 2 if n % 2 == 0 else 1
    chips = n // cores
    wide = 1
    while (wide + 1) ** 3 <= chips:
        wide += 1
    while chips % wide:
        wide -= 1
    return cores, wide, chips // wide


def gather_kernel(
    n, per_rank, histories,
    span_ids_hbm, lengths_hbm, near_hbm, far_hbm, queries_hbm, keys_hbm, values_hbm,
    kv, meta, q_rot,
    span_ids, lengths, near, far, queries, keys, load_sem, send_sem, recv_sem,
):
    cores, wide, deep = layout_of(n)
    me = lax.axis_index("seq")
    group = lax.axis_index("groups")
    c = lax.rem(me, cores)
    x = lax.rem(me // cores, wide)
    z = me // (cores * wide)
    items = per_rank + 1

    def at(zz, xx):
        return (zz * wide + xx) * cores + c

    loads = [
        pltpu.make_async_copy(src, dst, load_sem.at[i])
        for i, (src, dst) in enumerate([
            (span_ids_hbm, span_ids), (lengths_hbm, lengths), (far_hbm, far),
            (keys_hbm, keys), (near_hbm, near),
        ] + [
            (values_hbm.at[pl.ds(slot * SPAN, SPAN)],
             kv.at[me * per_rank + slot, :, pl.ds(HD, HD)])
            for slot in range(per_rank)
        ] + [(queries_hbm, queries)])
    ]
    for load in loads:
        load.start()

    barrier = pltpu.get_barrier_semaphore()
    neighbours = [
        (z < deep - 1, me + wide * cores),
        (z > 0, me - wide * cores),
        (x < wide - 1, me + cores),
        (x > 0, me - cores),
    ]
    if cores == 2:
        neighbours.append((None, me + 1 - 2 * c))
    greeted = jnp.int32(0)
    for there, other in neighbours:
        def greet(other=other):
            pl.semaphore_signal(barrier, inc=1, device_id=(group, other), device_id_type=MESH)
        if there is None:
            greet()
            greeted = greeted + 1
        else:
            pl.when(there)(greet)
            greeted = greeted + there.astype(jnp.int32)

    for load in loads[:-1]:
        load.wait()

    factors = []
    for slot in range(per_rank):
        span = span_ids[slot]
        place = span - start_of(span, lengths, histories)
        base = far[pl.ds(place, 1)]
        c2, s2 = base[0, 0:1, :], base[0, 1:2, :]
        c1, s1 = near[0], near[1]
        factors.append((c1 * c2 - s1 * s2, s1 * c2 + c1 * s2))

    def rotate(rows, slot):
        cosine, sine = factors[slot]
        rows = rows.astype(jnp.float32)
        return (rows * cosine + pltpu.roll(rows, HD // 2, 1) * sine).astype(jnp.bfloat16)

    lane = lax.broadcasted_iota(jnp.int32, (1, 128), 1)
    note = jnp.zeros((1, 128), jnp.int32)
    for slot in range(per_rank):
        note = jnp.where(lane == slot, span_ids[slot], note)
    meta[me] = note
    for slot in range(per_rank):
        rows = slice(slot * SPAN, (slot + 1) * SPAN)
        kv[me * per_rank + slot, :, :HD] = rotate(keys[rows, :], slot)

    pl.semaphore_wait(barrier, greeted)

    def ref_of(device, k):
        return kv.at[device * per_rank + k] if k < per_rank else meta.at[device]

    pending = []

    def both(a, b):
        return a if b is None else (b if a is None else jnp.logical_and(a, b))

    def send(device, k, target, there):
        number = len(pending)
        ref = ref_of(device, k)
        copy = pltpu.make_async_remote_copy(
            src_ref=ref, dst_ref=ref,
            send_sem=send_sem.at[number], recv_sem=recv_sem.at[device * items + k],
            device_id=(group, target), device_id_type=MESH,
        )
        if there is None:
            copy.start()
            pending.append((None, copy))
        else:
            pl.when(there)(copy.start)
            pending.append((there, copy))

    def arrive(device, k, there):
        ref = ref_of(device, k)
        copy = pltpu.make_async_remote_copy(
            src_ref=ref, dst_ref=ref,
            send_sem=send_sem.at[0], recv_sem=recv_sem.at[device * items + k],
            device_id=(group, me), device_id_type=MESH,
        )
        if there is None:
            copy.wait_recv()
        else:
            pl.when(there)(copy.wait_recv)

    def up(device, k, there):
        send(device, k, me + wide * cores, both(there, z < deep - 1))

    def down(device, k, there):
        send(device, k, me - wide * cores, both(there, z > 0))

    def right(device, k, there):
        send(device, k, me + cores, both(there, x < wide - 1))

    def left(device, k, there):
        send(device, k, me - cores, both(there, x > 0))

    def partner(device, k, there):
        if cores == 2:
            send(device, k, me + 1 - 2 * c, there)

    balanced = wide == 2 and deep >= 4
    late = per_rank - 1

    for k in range(items):
        down(me, k, None)
        up(me, k, None)
        right(me, k, None)
        left(me, k, None)
    for k in range(items):
        partner(me, k, None)

    loads[-1].wait()
    for slot in range(per_rank):
        rows = slice(slot * SPAN, (slot + 1) * SPAN)
        for head in range(QH):
            q_rot[slot, head * SPAN:(head + 1) * SPAN, :] = rotate(
                queries[rows, head * HD:(head + 1) * HD], slot
            )

    for d in range(deep):
        if d < deep - 1:
            far_by = d + 1
            for k in range(items):
                for sign in (1, -1):
                    row = z + sign * far_by
                    there = row >= 0 if sign < 0 else row < deep
                    device = at(row, x)
                    arrive(device, k, there)
                    (up if sign < 0 else down)(device, k, there)
                    across = there
                    if balanced and k == late:
                        along = jnp.logical_or(row == 0, row == deep - 1)
                        across = jnp.logical_and(there, jnp.logical_not(along))
                    right(device, k, across)
                    left(device, k, across)
                    partner(device, k, there)
        for k in range(items):
            for sign in ((1, -1) if d else (1,)):
                row = z + sign * d
                row_there = None if d == 0 else (row >= 0 if sign < 0 else row < deep)
                for e in range(1, wide):
                    for side in (-1, 1):
                        column = x + side * e
                        there = both(row_there, column >= 0 if side < 0 else column < wide)
                        device = at(row, column)
                        arrive(device, k, there)
                        if e < wide - 1:
                            (right if side < 0 else left)(device, k, there)
                        if balanced and k == late:
                            if d == 0 or sign < 0:
                                up(device, k, both(there, row == 0))
                            if d == 0 or sign > 0:
                                down(device, k, both(there, row == deep - 1))
                        partner(device, k, there)

    if cores == 2:
        def drain(chip, carry):
            device = chip * cores + 1 - c
            for k in range(items):
                arrive(device, k, None)
            return carry

        lax.fori_loop(0, n // cores, drain, 0)
    for there, copy in pending:
        if there is None:
            copy.wait_send()
        else:
            pl.when(there)(copy.wait_send)


def sends_of(n, per_rank):
    cores, wide, deep = layout_of(n)
    items = per_rank + 1
    total = items * 5 + items * 2 * (deep - 1) * 4
    total += items * (2 * deep - 1) * 2 * (wide - 1) * 4
    return total


def attend_kernel(
    per_rank, span_total, histories, tile, axis,
    span_ids_hbm, lengths_hbm, page_dest_hbm, meta, q_rot, kv,
    context, paged,
    span_ids, lengths, page_dest, load_sem, where_is, scores, best, total, accum,
):
    loads = [
        pltpu.make_async_copy(src, dst, load_sem.at[i])
        for i, (src, dst) in enumerate([
            (span_ids_hbm, span_ids), (lengths_hbm, lengths), (page_dest_hbm, page_dest),
        ])
    ]
    for load in loads:
        load.start()
    rank = lax.axis_index(axis)
    devices = span_total // per_rank
    gain = math.log2(math.e) / math.sqrt(HD)

    for device in range(devices):
        for k in range(per_rank):
            where_is[meta[device, 0, k]] = device * per_rank + k

    for load in loads:
        load.wait()
    for slot in range(per_rank):
        wanted = rank * per_rank + slot
        found = jnp.int32(0)
        for j in range(span_total):
            found = jnp.where(page_dest[j] == wanted, j, found)
        paged[slot] = kv[where_is[found]]

    def joined(cur, first, width, columns):
        blocks = [kv[where_is[cur - first - j], :, columns] for j in range(width)]
        return blocks[0] if width == 1 else jnp.concatenate(blocks, axis=0)

    def one(item, carry):
        slot = item // (QH * SPAN // tile)
        row0 = pl.multiple_of(lax.rem(item, QH * SPAN // tile) * tile, tile)
        cur = span_ids[slot]
        behind = cur - start_of(cur, lengths, histories)
        eights = behind // 8
        fours = lax.rem(behind, 8) // 4
        twos = lax.rem(behind, 4) // 2
        ones = lax.rem(behind, 2)
        query = q_rot[slot, pl.ds(row0, tile), :]

        def dots(first, width):
            return lax.dot_general(
                query, joined(cur, first, width, slice(0, HD)),
                (((1,), (1,)), ((), ())), preferred_element_type=jnp.float32,
            )

        def score(first, width):
            block = dots(first, width)
            top = best[...]
            for j in range(width):
                piece = block[:, j * SPAN:(j + 1) * SPAN]
                scores[first + j] = piece
                top = jnp.maximum(top, piece)
            best[...] = top

        def weigh(first, width, fresh=False):
            top = best[...]
            parts, summed = [], None
            for j in range(width):
                part = jnp.exp2((scores[first + j] - top) * gain)
                summed = part if summed is None else summed + part
                parts.append(part.astype(jnp.bfloat16))
            low = parts[0] if width == 1 else jnp.concatenate(parts, axis=1)
            mixed = jnp.dot(
                low, joined(cur, first, width, slice(HD, 2 * HD)), preferred_element_type=jnp.float32
            )
            if fresh:
                total[...] = summed
                accum[...] = mixed
            else:
                total[...] += summed
                accum[...] += mixed

        def sweep(step):
            def body(i, c):
                step(1 + i * 8, 8)
                return c

            lax.fori_loop(0, eights, body, 0)

            @pl.when(fours == 1)
            def _():
                step(1 + eights * 8, 4)

            @pl.when(twos == 1)
            def _():
                step(1 + eights * 8 + fours * 4, 2)

            @pl.when(ones == 1)
            def _():
                step(1 + eights * 8 + fours * 4 + twos * 2, 1)

        own = dots(0, 1)
        row = lax.rem(lax.broadcasted_iota(jnp.int32, (tile, SPAN), 0), SPAN)
        col = lax.broadcasted_iota(jnp.int32, (tile, SPAN), 1)
        own = jnp.where(col <= row, own, NEG)
        scores[0] = own
        best[...] = own
        sweep(score)
        best[...] = jnp.broadcast_to(jnp.max(best[...], axis=1, keepdims=True), (tile, SPAN))
        weigh(0, 1, fresh=True)
        sweep(weigh)
        result = accum[...] / jnp.sum(total[...], axis=1, keepdims=True)
        result = result.astype(jnp.bfloat16)
        rows = pl.ds(pl.multiple_of(slot * SPAN, SPAN), SPAN)
        heads = tile // SPAN
        if heads == QH:
            for head in range(QH):
                context[rows, head * HD:(head + 1) * HD] = result[head * SPAN:(head + 1) * SPAN]
        else:
            for head in range(heads):
                place = pl.ds(pl.multiple_of(row0 // SPAN * HD + head * HD, HD), HD)
                context[rows, place] = result[head * SPAN:(head + 1) * SPAN]
        return carry

    lax.fori_loop(0, per_rank * (QH * SPAN // tile), one, 0)


def in_hbm(array):
    return pltpu.with_memory_space_constraint(array, pltpu.HBM)


def on_device(n, queries, keys, values, span_ids, lengths, page_dest):
    per_rank = span_ids.shape[0]
    span_total = page_dest.shape[0]
    histories = lengths.shape[0]
    near, far = tables(span_total)
    vmem, smem = pl.BlockSpec(memory_space=VMEM), pl.BlockSpec(memory_space=SMEM)
    hbm = pl.BlockSpec(memory_space=pltpu.HBM)
    gathered = span_total * SPAN * 2 * HD * 2
    items = per_rank + 1
    kv, meta, q_rot = pl.pallas_call(
        functools.partial(gather_kernel, n, per_rank, histories),
        out_shape=(
            jax.ShapeDtypeStruct((span_total, SPAN, 2 * HD), jnp.bfloat16),
            jax.ShapeDtypeStruct((n, 1, 128), jnp.int32),
            jax.ShapeDtypeStruct((per_rank, QH * SPAN, HD), jnp.bfloat16),
        ),
        in_specs=[hbm] * 7,
        out_specs=(vmem, vmem, vmem),
        scratch_shapes=[
            SMEM(span_ids.shape, jnp.int32),
            SMEM(lengths.shape, jnp.int32),
            VMEM(near.shape, jnp.float32),
            VMEM(far.shape, jnp.float32),
            VMEM(queries.shape, jnp.bfloat16),
            VMEM(keys.shape, jnp.bfloat16),
            pltpu.SemaphoreType.DMA((6 + per_rank,)),
            pltpu.SemaphoreType.DMA((sends_of(n, per_rank),)),
            pltpu.SemaphoreType.DMA((n * items,)),
        ],
        compiler_params=pltpu.CompilerParams(
            collective_id=0, has_side_effects=True, vmem_limit_bytes=gathered + 6 * 2**20
        ),
        name="gather",
    )(*map(in_hbm, (span_ids, lengths, jnp.asarray(near), jnp.asarray(far), queries, keys, values)))
    reach = span_total // 2
    tile = QH * SPAN
    for parts in (1, 2, 3, 6):
        tile = QH * SPAN // parts
        if tile * reach * SPAN * 4 <= 16 * 2**20:
            break
    return pl.pallas_call(
        functools.partial(attend_kernel, per_rank, span_total, histories, tile, "seq"),
        out_shape=(
            jax.ShapeDtypeStruct(queries.shape, jnp.bfloat16),
            jax.ShapeDtypeStruct((per_rank, SPAN, 2 * HD), jnp.bfloat16),
        ),
        in_specs=[hbm, hbm, hbm, smem, vmem, vmem],
        out_specs=(vmem, vmem),
        scratch_shapes=[
            SMEM(span_ids.shape, jnp.int32),
            SMEM(lengths.shape, jnp.int32),
            SMEM(page_dest.shape, jnp.int32),
            pltpu.SemaphoreType.DMA((3,)),
            SMEM((span_total,), jnp.int32),
            VMEM((reach, tile, SPAN), jnp.float32),
            VMEM((tile, SPAN), jnp.float32),
            VMEM((tile, SPAN), jnp.float32),
            VMEM((tile, HD), jnp.float32),
        ],
        compiler_params=pltpu.CompilerParams(vmem_limit_bytes=gathered + 24 * 2**20),
        name="attend",
    )(*map(in_hbm, (span_ids, lengths, page_dest)), meta, q_rot, kv)


def solution(mesh):
    rows = P(("groups", "seq"), None)
    return jax.shard_map(
        functools.partial(on_device, mesh.shape["seq"]),
        mesh=mesh,
        in_specs=(rows, rows, rows, P(("groups", "seq")), P("groups"), P("groups")),
        out_specs=(rows, P(("groups", "seq"), None, None)),
        check_vma=False,
    )
```
